512 devices in a mesh: rows: 512 (over y, z, x, core).
Axes of the slice: x: 4, y: 4, z: 16, core: 2. Of those that a mesh axis runs over, the one named last changes fastest.
Arguments:
- coupling: float32 [2048, 5, 128, 128], P('rows'), may hold values from -0.15 to 3.15, as said below
- columns: int32 [2048, 5], replicated, may hold values from 0 to 1023, as said below
- row_slots: int32 [1024], replicated, may hold values from 0 to 2047, as said below
Outputs:
- inverse_estimate: float32 [2048, 5, 128, 128], P('rows')
The draws below stay inside these ranges and needn't reach their ends.
Inputs may be any that keep to these rules, and one draw needn't show every extreme that they name: `coupling`: in every slot the diagonal entries of tile 0 are at least 0.3. `columns`: for a slot that holds block row r, entry 0 is r and the other 4 entries are distinct block rows (r + d) mod 1024 with 1 <= |d| <= 3; entries of slots that hold no block row mean nothing. `row_slots`: device i owns slots i * 4 to (i + 1) * 4 - 1. Block rows are owned in order: device 0 holds the first ones, each device a contiguous run of rows in its first slots, at least 1 and at most 4 rows; some device holds 4.
All inputs are finite; a program needn't handle non-finite values.
Results may differ from the reference program's by a relative error of at most 0.0003.
Values sent between devices are 32-bit elements; how exact they have to be, the bound alone decides.
A program may use at most 64 MiB of HBM per device.

```python
import math
import jax
import jax.numpy as jnp
import numpy as np
from jax import lax

TILE = 128
ROW_TILES = 5
BAND = 3
ROWS_DEV = 2
SLOT_DEV = 4
BLOCK_ROWS = 1024
SLOTS = 2048


def layout(key):
    devices = BLOCK_ROWS // ROWS_DEV
    quads = devices // 4
    key_kind, key_order, key_pick, key_fill = jax.random.split(jax.random.fold_in(key, 7), 4)
    table = jnp.array(np.array([[4, 2, 1, 1], [3, 3, 1, 1], [2, 2, 2, 2], [3, 2, 2, 1]], np.int32))
    kinds = jax.random.randint(key_kind, (quads,), 0, 4).at[0].set(0)
    units = jnp.take(table, kinds, axis=0)
    scores = jax.random.randint(key_order, (quads, 4), 0, 1024) * 4 + jnp.arange(4, dtype=jnp.int32)
    units = jnp.take_along_axis(units, jnp.argsort(scores, axis=1), axis=1)
    counts = units.reshape(-1) * (ROWS_DEV // 2)
    starts = jnp.cumsum(counts) - counts
    every_row = jnp.arange(BLOCK_ROWS, dtype=jnp.int32)
    owners = jnp.sum((starts[None, :] <= every_row[:, None]).astype(jnp.int32), axis=1) - 1
    row_slots = owners * SLOT_DEV + every_row - jnp.take(starts, owners)
    reach = jnp.concatenate([jnp.arange(-BAND, 0), jnp.arange(1, BAND + 1)]).astype(jnp.int32)
    picks = jax.random.randint(key_pick, (BLOCK_ROWS, 2 * BAND), 0, 1 << 20) * (2 * BAND) + jnp.arange(2 * BAND, dtype=jnp.int32)
    chosen = jnp.argsort(picks, axis=1)[:, :ROW_TILES - 1]
    neighbours = (every_row[:, None] + jnp.take(reach, chosen)) % BLOCK_ROWS
    row_columns = jnp.concatenate([every_row[:, None], neighbours], axis=1)
    filler = jax.random.randint(key_fill, (SLOTS, ROW_TILES), 0, BLOCK_ROWS)
    columns = filler.at[row_slots].set(row_columns)
    return (columns, row_slots)


def draw_columns(key, part):
    return layout(key)[0]


def draw_row_slots(key, part):
    return layout(key)[1]


def draw_coupling(key, part):
    key_off, key_diag = jax.random.split(jax.random.fold_in(key, 3))
    shape = (SLOTS, ROW_TILES, TILE, TILE)
    deviation = 0.11 / math.sqrt(TILE)
    spread = jnp.clip(jax.random.normal(key_off, shape, jnp.float32), -6.0, 6.0) * deviation
    scales = jnp.exp(jax.random.uniform(key_diag, (SLOTS, TILE), jnp.float32, math.log(0.5), math.log(2.0)))
    identity = jnp.eye(TILE, dtype=jnp.float32)
    leading = (jnp.arange(ROW_TILES) == 0).astype(jnp.float32)
    return spread + leading[None, :, None, None] * scales[:, None, :, None] * identity


def setup_inputs(seed: int = 0) -> dict:
    arg_keys = jax.random.split(jax.random.key(seed), 4)
    return {
        "coupling": draw_coupling(jax.random.fold_in(arg_keys[3], 71), 0),
        "columns": draw_columns(jax.random.fold_in(arg_keys[3], 71), 0),
        "row_slots": draw_row_slots(jax.random.fold_in(arg_keys[3], 71), 0),
    }


precise = lax.Precision.HIGHEST


def locate(wanted, row_ids):
    matches = wanted[..., None] == row_ids
    return jnp.argmax(matches, axis=-1).astype(jnp.int32)


def start_iterate(coupling, inverse, column_inverse):
    identity = jnp.eye(coupling.shape[-1], dtype=coupling.dtype)
    leading = (jnp.arange(coupling.shape[1]) == 0).astype(coupling.dtype)
    diagonal_part = 2.0 * leading[None, :, None, None] * (inverse[:, None, :, None] * identity)
    return diagonal_part - inverse[:, None, :, None] * coupling * column_inverse[:, :, None, :]


def pattern_product(left, row_pool, row_ids, pool_columns, own_columns):
    def per_slot(operands):
        blocks, row_columns = operands
        located = locate(row_columns, row_ids)
        fetched = jnp.take(row_pool, located, axis=0)
        their_columns = jnp.take(pool_columns, located, axis=0)
        selector = (their_columns[:, :, None] == row_columns[None, None, :]).astype(row_pool.dtype)
        chosen = jnp.einsum("kab,kaqr->kbqr", selector, fetched, precision=precise)
        return jnp.einsum("kpq,kbqr->bpr", blocks, chosen, precision=precise)

    return lax.map(per_slot, (left, own_columns))


def reference(coupling, columns, row_slots):
    blocks = jnp.take(coupling, row_slots, axis=0)
    row_columns = jnp.take(columns, row_slots, axis=0)
    inverse = 1.0 / jnp.diagonal(blocks[:, 0], axis1=1, axis2=2)
    column_inverse = jnp.take(inverse, row_columns, axis=0)
    first_iterate = start_iterate(blocks, inverse, column_inverse)
    every_row = jnp.arange(BLOCK_ROWS, dtype=jnp.int32)
    product = pattern_product(blocks, first_iterate, every_row, row_columns, row_columns)
    second_iterate = 2.0 * first_iterate - pattern_product(first_iterate, product, every_row, row_columns, row_columns)
    return jnp.zeros_like(coupling).at[row_slots].set(second_iterate)
```

```python
import functools

import jax
import jax.numpy as jnp
from jax import lax
from jax.experimental import pallas as pl
from jax.experimental.pallas import tpu as pltpu
from jax.sharding import PartitionSpec as P

TILE = 128
TILES = 5
SLOT = 4
BAND = 3
AXIS = "rows"
MESH = pl.DeviceIdType.MESH

WIDTHS = (5, 5, 5, 3, 2, 1)


def first_row(slots_ref, bound):
    found = jnp.int32(0)
    step = slots_ref.shape[0] // 2
    while step:
        below = slots_ref[found + step - 1] < bound
        found = found + jnp.where(below, step, 0)
        step //= 2
    return found


def ownership(slots_ref, me):
    rows = slots_ref.shape[0]
    start = first_row(slots_ref, me * SLOT)
    count = jnp.int32(1)
    for k in range(1, SLOT):
        at = start + k
        inside = slots_ref[jnp.minimum(at, rows - 1)] < (me + 1) * SLOT
        count = count + jnp.where(jnp.logical_and(at < rows, inside), 1, 0)
    return start, count


def wrapped(value, rows):
    return lax.rem(value + rows, rows)


def signed(value, rows):
    half = rows // 2
    return lax.rem(value + rows + half, rows) - half


def diagonal_mask():
    shape = (TILE, TILE)
    return lax.broadcasted_iota(jnp.int32, shape, 0) == lax.broadcasted_iota(jnp.int32, shape, 1)


def inverse_column(tile, eye):
    return 1.0 / jnp.sum(jnp.where(eye, tile, 0.0), axis=1, keepdims=True)


def inverse_row(tile, eye):
    return 1.0 / jnp.sum(jnp.where(eye, tile, 0.0), axis=0, keepdims=True)


def tile_at_offset(slots_ref, columns_ref, row, offset, rows):
    slot = slots_ref[row]
    target = wrapped(row + offset, rows)
    found = jnp.int32(0)
    for v in range(1, TILES):
        found = jnp.where(columns_ref[v, slot] == target, v, found)
    return found


def exchange_kernel(devices, own_ref, columns_ref, slots_ref, *refs):
    before, after = refs[0:6], refs[6:12]
    send_before, send_after = refs[12:18], refs[18:24]
    send_sem, recv_sem = refs[24], refs[25]
    rows = slots_ref.shape[0]
    me = lax.axis_index(AXIS)
    right, left = lax.rem(me + 1, devices), lax.rem(me + devices - 1, devices)

    barrier = pltpu.get_barrier_semaphore()
    for other in (left, right):
        pl.semaphore_signal(barrier, inc=1, device_id=(other,), device_id_type=MESH)

    start, count = ownership(slots_ref, me)
    eye = diagonal_mask()

    pl.semaphore_wait(barrier, 2)

    def copy(side, k):
        source = (send_before, send_after)[side][k]
        if side == 1 and k == 0:
            source = own_ref.at[0]
        return pltpu.make_async_remote_copy(
            src_ref=source,
            dst_ref=(before, after)[side][k],
            send_sem=send_sem.at[side, k],
            recv_sem=recv_sem.at[side, k],
            device_id=((right, left)[side],),
            device_id_type=MESH,
        )

    def own_slot(side, k):
        return jnp.maximum(count - 1 - k, 0) if side == 0 else k

    def fill_whole(side, k):
        received = (before, after)[side]
        target = (send_before, send_after)[side][k]
        for t in range(TILES):
            value = own_ref[own_slot(side, k), t]
            for held in range(1, k + 1):
                value = jnp.where(count == held, received[k - held][t], value)
            target[t] = value

    def fill_part(side, k):
        received = (before, after)[side]
        target = (send_before, send_after)[side][k]
        sign = 1 if side == 0 else -1
        row = wrapped(start + count - 1 - k if side == 0 else start + k, rows)
        diagonal = None
        for held in range(1, SLOT + 1):
            position = k - held
            if position == -1 or position > 2:
                continue
            tile = received[position][0]
            diagonal = tile if diagonal is None else jnp.where(count == held, tile, diagonal)
        if k == 3:
            diagonal = jnp.where(count == SLOT, own_ref[own_slot(side, k), 0], diagonal)
        scale = inverse_column(diagonal, eye)
        for place in range(WIDTHS[k]):
            offset = sign * (BAND - WIDTHS[k] + 1 + place)
            index = tile_at_offset(slots_ref, columns_ref, row, offset, rows)
            value = own_ref[own_slot(side, k), index] if k == 3 else None
            for held in range(1, SLOT + 1):
                position = k - held
                if position > 2 or position < 0:
                    continue
                tile = received[position][index]
                value = tile if value is None else jnp.where(count == held, tile, value)
            value = jnp.where(index > 0, -(scale * value), 0.0)
            for held in range(1, SLOT + 1):
                position = k - held
                if position > 2:
                    ready = received[position][WIDTHS[position] - WIDTHS[k] + place]
                    value = jnp.where(count == held, ready, value)
            target[place] = value

    for k in range(6):
        for side in (0, 1):
            if k > 0:
                copy(side, k - 1).wait_recv()
            if k < 3:
                if not (side == 1 and k == 0):
                    fill_whole(side, k)
            else:
                fill_part(side, k)
            copy(side, k).start()
    for side in (0, 1):
        copy(side, 5).wait_recv()
    for side in (0, 1):
        for k in range(6):
            copy(side, k).wait_send()


def exchange(devices, own, columns, slots):
    windows = [(w, TILE, TILE) for w in WIDTHS] * 2
    vmem = pl.BlockSpec(memory_space=pltpu.VMEM)
    smem = pl.BlockSpec(memory_space=pltpu.SMEM)
    return pl.pallas_call(
        functools.partial(exchange_kernel, devices),
        out_shape=[jax.ShapeDtypeStruct(w, jnp.float32) for w in windows],
        in_specs=[vmem, smem, smem],
        out_specs=[vmem] * 12,
        scratch_shapes=[pltpu.VMEM(w, jnp.float32) for w in windows]
        + [pltpu.SemaphoreType.DMA((2, 6)), pltpu.SemaphoreType.DMA((2, 6))],
        compiler_params=pltpu.CompilerParams(collective_id=0, has_side_effects=True),
        name="exchange",
    )(own, columns, slots)


WHOLE = 10 * TILES
PARTS = (3, 2, 1)
ZERO = WHOLE + 2 * sum(PARTS)
PLACES = 16
SPAN = 2 * BAND + 1


def whole_place(f):
    return 6 + f if f < 4 else (9 - f if f < 7 else 3 + f)


def split(value):
    high = value.astype(jnp.bfloat16)
    low = (value - high.astype(jnp.float32)).astype(jnp.bfloat16)
    return high, low


def multiply(left_high, left_low, base, pool_high, pool_low, table_ref):
    chunks = ((0, 1), (2, 3), (4,))

    def block(pool, us, ts):
        return jnp.concatenate(
            [
                jnp.concatenate([pool[table_ref[u * TILES + t]] for t in ts], axis=1)
                for u in us
            ],
            axis=0,
        )

    out = []
    for ts in chunks:
        total = None
        rest = None
        for us in chunks:
            high = jnp.concatenate([left_high[base + u] for u in us], axis=1)
            low = jnp.concatenate([left_low[base + u] for u in us], axis=1)
            both = jnp.concatenate([high, low], axis=0)
            part = jnp.dot(both, block(pool_high, us, ts), preferred_element_type=jnp.float32)
            more = jnp.dot(high, block(pool_low, us, ts), preferred_element_type=jnp.float32)
            total = part if total is None else total + part
            rest = more if rest is None else rest + more
        value = total[:TILE] + total[TILE:] + rest
        for n in range(len(ts)):
            out.append(value[:, n * TILE : (n + 1) * TILE])
    return out


def iterate_kernel(own_ref, columns_ref, slots_ref, *refs):
    before, after = refs[0:6], refs[6:12]
    out_ref = refs[12]
    e_high, e_low, f_high, f_low, inverses, tiles, offsets, where = refs[13:]
    rows = slots_ref.shape[0]
    me = lax.axis_index(AXIS)
    start, count = ownership(slots_ref, me)
    eye = diagonal_mask()

    def distance(f):
        if f < 4:
            return jnp.int32(f)
        return jnp.int32(3 - f) if f < 7 else count + (f - 7)

    def place_of(d):
        return 6 + d + jnp.where(d < count, 0, SLOT - count)

    @pl.loop(0, PLACES * SPAN)
    def _(i):
        tiles[i] = ZERO

    for side in (0, 1):
        at = WHOLE + side * sum(PARTS)
        for k in range(3):
            place = 2 - k if side == 0 else 13 + k
            for n in range(PARTS[k]):
                offset = (BAND - PARTS[k] + 1 + n) * (1 if side == 0 else -1)
                tiles[place * SPAN + BAND + offset] = at
                value = (before, after)[side][3 + k][n]
                e_high[at], e_low[at] = split(value)
                at += 1
    e_high[ZERO] = jnp.zeros((TILE, TILE), jnp.bfloat16)
    e_low[ZERO] = jnp.zeros((TILE, TILE), jnp.bfloat16)
    f_high[ZERO] = jnp.zeros((TILE, TILE), jnp.bfloat16)
    f_low[ZERO] = jnp.zeros((TILE, TILE), jnp.bfloat16)

    for f in range(10):
        source = own_ref.at[f] if f < 4 else (before[f - 4] if f < 7 else after[f - 7])
        row = wrapped(start + distance(f), rows)
        slot = slots_ref[row]
        for v in range(TILES):
            offset = signed(columns_ref[v, slot] - row, rows)
            offsets[f * TILES + v] = offset
            tiles[whole_place(f) * SPAN + BAND + offset] = f * TILES + v
        diagonal = source[0]
        scale = inverse_column(diagonal, eye)
        inverses[whole_place(f)] = jnp.broadcast_to(inverse_row(diagonal, eye), (8, TILE))
        for v in range(TILES):
            value = -(scale * source[v])
            if v == 0:
                value = jnp.where(eye, 1.0, 0.0) + value
            e_high[f * TILES + v], e_low[f * TILES + v] = split(value)

    def name_tiles(f, d):
        for u in range(TILES):
            place = place_of(d + offsets[f * TILES + u])
            for t in range(TILES):
                offset = offsets[f * TILES + t] - offsets[f * TILES + u]
                near = jnp.logical_and(offset <= BAND, offset >= -BAND)
                at = place * SPAN + BAND + jnp.where(near, offset, 0)
                where[u * TILES + t] = jnp.where(near, tiles[at], ZERO)

    @pl.loop(0, 10)
    def _(f):
        d = jnp.where(f < 4, f, jnp.where(f < 7, 3 - f, count + (f - 7)))

        @pl.when(jnp.logical_or(f >= 4, f < count))
        def _():
            name_tiles(f, d)
            made = multiply(e_high, e_low, f * TILES, e_high, e_low, where)
            for t in range(TILES):
                f_high[f * TILES + t], f_low[f * TILES + t] = split(made[t])

    @pl.loop(0, SLOT)
    def _(f):
        @pl.when(f < count)
        def _():
            name_tiles(f, f)
            made = multiply(e_high, e_low, f * TILES, f_high, f_low, where)
            diagonal = own_ref[f, 0]
            scale = inverse_column(diagonal, eye)
            for t in range(TILES):
                value = -(scale * own_ref[f, t])
                if t == 0:
                    value = jnp.where(eye, 2.0, 0.0) + value
                at = f * TILES + t
                second = f_high[at].astype(jnp.float32) + f_low[at].astype(jnp.float32)
                value = value + (second + made[t])
                place = place_of(f + offsets[at])
                out_ref[f, t] = value * inverses[place][0:1]

        @pl.when(f >= count)
        def _():
            out_ref[f] = jnp.zeros((TILES, TILE, TILE), jnp.float32)


def iterate(own, columns, slots, windows):
    vmem = pl.BlockSpec(memory_space=pltpu.VMEM)
    smem = pl.BlockSpec(memory_space=pltpu.SMEM)
    pool = pltpu.VMEM((ZERO + 1, TILE, TILE), jnp.bfloat16)
    return pl.pallas_call(
        iterate_kernel,
        out_shape=jax.ShapeDtypeStruct(own.shape, own.dtype),
        in_specs=[vmem, smem, smem] + [vmem] * 12,
        out_specs=vmem,
        scratch_shapes=[pool] * 4
        + [
            pltpu.VMEM((PLACES, 8, TILE), jnp.float32),
            pltpu.SMEM((PLACES * SPAN,), jnp.int32),
            pltpu.SMEM((10 * TILES,), jnp.int32),
            pltpu.SMEM((TILES * TILES,), jnp.int32),
        ],
        name="iterate",
    )(own, columns, slots, *windows)


def shards(coupling, columns, row_slots):
    devices = lax.axis_size(AXIS)
    by_tile = columns.T
    windows = exchange(devices, coupling, by_tile, row_slots)
    return iterate(coupling, by_tile, row_slots, windows)


def solution(mesh):
    return jax.shard_map(
        shards,
        mesh=mesh,
        in_specs=(P(AXIS, None, None, None), P(), P()),
        out_specs=P(AXIS, None, None, None),
        check_vma=False,
    )
```

```python
import functools

import jax
import jax.numpy as jnp
from jax import lax
from jax.experimental import pallas as pl
from jax.experimental.pallas import tpu as pltpu
from jax.sharding import PartitionSpec as P

TILE = 128
TILES = 5
SLOT = 4
BAND = 3
AXIS = "rows"
MESH = pl.DeviceIdType.MESH

WIDTHS = (5, 5, 5, 3, 2, 1)

WHOLE = 10 * TILES
PARTS = WIDTHS[3:]
ZERO = WHOLE + 2 * sum(PARTS)
PLACES = 16
SPAN = 2 * BAND + 1
NAMES = TILES * TILES


def first_row(slots_ref, bound):
    found = jnp.int32(0)
    step = slots_ref.shape[0] // 2
    while step:
        below = slots_ref[found + step - 1] < bound
        found = found + jnp.where(below, step, 0)
        step //= 2
    return found


def ownership(slots_ref, me):
    rows = slots_ref.shape[0]
    start = first_row(slots_ref, me * SLOT)
    count = jnp.int32(1)
    for k in range(1, SLOT):
        at = start + k
        inside = slots_ref[jnp.minimum(at, rows - 1)] < (me + 1) * SLOT
        count = count + jnp.where(jnp.logical_and(at < rows, inside), 1, 0)
    return start, count


def wrapped(value, rows):
    return lax.rem(value + rows, rows)


def signed(value, rows):
    half = rows // 2
    return lax.rem(value + rows + half, rows) - half


def inverse_column(tile, eye):
    return 1.0 / jnp.sum(jnp.where(eye, tile, 0.0), axis=1, keepdims=True)


def inverse_row(tile, eye):
    return 1.0 / jnp.sum(jnp.where(eye, tile, 0.0), axis=0, keepdims=True)


def split(value):
    high = value.astype(jnp.bfloat16)
    low = (value - high.astype(jnp.float32)).astype(jnp.bfloat16)
    return high, low


def dot(left, right):
    return jnp.dot(left, right, preferred_element_type=jnp.float32)


def multiply(left_high, left_low, base, pool_high, pool_low, names_ref, named):
    def block(pool, us, ts):
        return jnp.concatenate(
            [
                jnp.concatenate([pool[names_ref[named + u * TILES + t]] for t in ts], axis=1)
                for u in us
            ],
            axis=0,
        )

    def left(us):
        high = jnp.concatenate([left_high[base + u] for u in us], axis=1)
        low = jnp.concatenate([left_low[base + u] for u in us], axis=1)
        return high, jnp.concatenate([high, low], axis=0)

    pairs = ((0, 1), (2, 3))
    out = []
    for ts in pairs:
        total = None
        rest = None
        for us in pairs:
            high, both = left(us)
            part = dot(both, block(pool_high, us, ts))
            more = dot(high, block(pool_low, us, ts))
            total = part if total is None else total + part
            rest = more if rest is None else rest + more
        high = left_high[base + 4]
        low = left_low[base + 4]
        last = jnp.concatenate(
            [
                jnp.concatenate([high, high], axis=1),
                jnp.concatenate([low, jnp.zeros_like(low)], axis=1),
            ],
            axis=0,
        )
        right = jnp.concatenate([block(pool_high, (4,), ts), block(pool_low, (4,), ts)], axis=0)
        total = total + dot(last, right)
        value = total[:TILE] + total[TILE:] + rest
        out.append(value[:, :TILE])
        out.append(value[:, TILE:])
    total = None
    for us in pairs + ((4,),):
        right = jnp.concatenate([block(pool_high, us, (4,)), block(pool_low, us, (4,))], axis=1)
        part = dot(left(us)[1], right)
        total = part if total is None else total + part
    out.append(total[:TILE, :TILE] + (total[TILE:, :TILE] + total[:TILE, TILE:]))
    return out


def kernel(devices, own_hbm, columns_hbm, slots_ref, out_ref, own_ref, columns_ref, *refs):
    arriving = (refs[0:6], refs[6:12])
    leaving = (refs[12:18], refs[18:24])
    e_high, e_low, f_high, f_low, inverses, tiles, offsets, names = refs[24:32]
    send_sem, recv_sem, own_sem, columns_sem = refs[32:]
    rows = slots_ref.shape[0]
    me = lax.axis_index(AXIS)
    right, left = lax.rem(me + 1, devices), lax.rem(me + devices - 1, devices)
    odd = lax.rem(me, 2) == 1
    outward = jnp.where(odd, right, left)
    partner = jnp.where(odd, left, right)
    heading = (jnp.where(odd, 1, -1), jnp.where(odd, -1, 1))

    barrier = pltpu.get_barrier_semaphore()
    for other in (left, right):
        pl.semaphore_signal(barrier, inc=1, device_id=(other,), device_id_type=MESH)
    fetch = pltpu.make_async_copy(own_hbm, own_ref, own_sem)
    fetch.start()
    fetch_columns = pltpu.make_async_copy(columns_hbm, columns_ref, columns_sem)
    fetch_columns.start()

    start, count = ownership(slots_ref, me)
    shape = (TILE, TILE)
    eye = lax.broadcasted_iota(jnp.int32, shape, 0) == lax.broadcasted_iota(jnp.int32, shape, 1)

    fetch.wait()
    pl.semaphore_wait(barrier, 2)

    def copy(side, k):
        return pltpu.make_async_remote_copy(
            src_ref=leaving[side][k],
            dst_ref=arriving[1 - side][k],
            send_sem=send_sem.at[side, k],
            recv_sem=recv_sem.at[1 - side, k],
            device_id=((outward, partner)[side],),
            device_id_type=MESH,
        )

    def await_row(side, k):
        copy(1 - side, k).wait_recv()

    def own_slot(side, k):
        return jnp.where(heading[side] > 0, jnp.maximum(count - 1 - k, 0), k)

    def fill_whole(side, k):
        received = arriving[side]
        target = leaving[side][k]
        for t in range(TILES):
            value = own_ref[own_slot(side, k), t]
            for held in range(1, k + 1):
                value = jnp.where(count == held, received[k - held][t], value)
            target[t] = value

    def tile_at_offset(row, offset):
        slot = slots_ref[row]
        target = wrapped(row + offset, rows)
        found = jnp.int32(0)
        for v in range(1, TILES):
            found = jnp.where(columns_ref[v, slot] == target, v, found)
        return found

    def fill_part(side, k):
        received = arriving[side]
        target = leaving[side][k]
        row = wrapped(jnp.where(heading[side] > 0, start + count - 1 - k, start + k), rows)
        whole = [(held, k - held) for held in range(1, SLOT + 1) if 0 <= k - held <= 2]
        diagonal = own_ref[own_slot(side, k), 0] if k == 3 else None
        for held, position in whole:
            tile = received[position][0]
            diagonal = tile if diagonal is None else jnp.where(count == held, tile, diagonal)
        scale = inverse_column(diagonal, eye)
        for place in range(WIDTHS[k]):
            offset = heading[side] * (BAND - WIDTHS[k] + 1 + place)
            index = tile_at_offset(row, offset)
            value = own_ref[own_slot(side, k), index] if k == 3 else None
            for held, position in whole:
                tile = received[position][index]
                value = tile if value is None else jnp.where(count == held, tile, value)
            value = jnp.where(index > 0, -(scale * value), 0.0)
            for held in range(1, SLOT + 1):
                position = k - held
                if position > 2:
                    ready = received[position][WIDTHS[position] - WIDTHS[k] + place]
                    value = jnp.where(count == held, ready, value)
            target[place] = value

    def forward(side, k):
        if k < 3:
            fill_whole(side, k)
        else:
            fill_part(side, k)
        copy(side, k).start()

    def distance(side, k):
        return jnp.where(heading[side] > 0, -1 - k, count + k)

    def place_of(d):
        below = jnp.where(odd, 6 + d, 9 - d)
        above = jnp.where(odd, 10 + d - count, 5 - d + count)
        return jnp.where(d < 0, below, jnp.where(d < count, 6 + d, above))

    def row_place(f):
        return 6 + f if f < 4 else (9 - f if f < 7 else 3 + f)

    def row_distance(f):
        return jnp.int32(f) if f < 4 else distance((f - 4) // 3, (f - 4) % 3)

    def convert_whole(f):
        source = own_ref.at[f] if f < 4 else arriving[(f - 4) // 3][(f - 4) % 3]
        diagonal = source[0]
        scale = inverse_column(diagonal, eye)
        inverses[row_place(f)] = jnp.broadcast_to(inverse_row(diagonal, eye), (8, TILE))
        for v in range(TILES):
            value = -(scale * source[v])
            if v == 0:
                value = jnp.where(eye, 1.0, 0.0) + value
            e_high[f * TILES + v], e_low[f * TILES + v] = split(value)

    def part_index(side, k):
        return WHOLE + side * sum(PARTS) + sum(PARTS[: k - 3])

    def convert_part(side, k):
        at = part_index(side, k)
        for n in range(WIDTHS[k]):
            e_high[at + n], e_low[at + n] = split(arriving[side][k][n])

    forward(0, 0)
    forward(1, 0)

    fetch_columns.wait()
    for f in range(10):
        row = wrapped(start + row_distance(f), rows)
        slot = slots_ref[row]
        found = [jnp.int32(ZERO)] * SPAN
        found[BAND] = jnp.int32(f * TILES)
        offsets[f * TILES] = 0
        for v in range(1, TILES):
            offset = jnp.clip(signed(columns_ref[v, slot] - row, rows), -BAND, BAND)
            offsets[f * TILES + v] = offset
            for o in range(SPAN):
                if o != BAND:
                    found[o] = jnp.where(offset == o - BAND, f * TILES + v, found[o])
        for o in range(SPAN):
            tiles[row_place(f) * SPAN + o] = found[o]
    for side in (0, 1):
        for k in range(3, 6):
            place = 5 - k if side == 0 else 10 + k
            for o in range(SPAN):
                tiles[place * SPAN + o] = ZERO
            for n in range(WIDTHS[k]):
                offset = heading[side] * (BAND - WIDTHS[k] + 1 + n)
                tiles[place * SPAN + BAND + offset] = part_index(side, k) + n

    @pl.loop(0, 10)
    def _(f):
        stream = jnp.where(f < 7, heading[0], heading[1])
        k = jnp.where(f < 7, f - 4, f - 7)
        d = jnp.where(f < 4, f, jnp.where(stream > 0, -1 - k, count + k))
        for u in range(TILES):
            first = offsets[f * TILES + u]
            place = place_of(d + first)
            for t in range(TILES):
                offset = offsets[f * TILES + t] - first
                near = jnp.logical_and(offset <= BAND, offset >= -BAND)
                at = place * SPAN + BAND + jnp.where(near, offset, 0)
                names[f * NAMES + u * TILES + t] = jnp.where(near, tiles[at], ZERO)

    zeros = jnp.zeros((TILE, TILE), jnp.bfloat16)
    for pool in (e_high, e_low, f_high, f_low):
        pool[ZERO] = zeros
    for f in range(4):
        convert_whole(f)

    for k in range(1, 4):
        for side in (0, 1):
            await_row(side, k - 1)
            forward(side, k)
            convert_whole(4 + 3 * side + k - 1)

    def square(f):
        made = multiply(e_high, e_low, f * TILES, e_high, e_low, names, f * NAMES)
        for t in range(TILES):
            f_high[f * TILES + t], f_low[f * TILES + t] = split(made[t])

    pl.loop(0, 2)(square)
    for k in (4, 5):
        for side in (0, 1):
            await_row(side, k - 1)
            forward(side, k)
            convert_part(side, k - 1)
        if k == 4:
            pl.loop(2, 4)(square)
        pl.loop(0, 2)(lambda side: square(4 + 3 * side + (k - 4)))
    for side in (0, 1):
        await_row(side, 5)
        convert_part(side, 5)
    pl.loop(0, 2)(lambda side: square(4 + 3 * side + 2))

    @pl.loop(0, SLOT)
    def _(f):
        made = multiply(e_high, e_low, f * TILES, f_high, f_low, names, f * NAMES)
        scale = inverse_column(own_ref[f, 0], eye)
        for t in range(TILES):
            value = -(scale * own_ref[f, t])
            if t == 0:
                value = jnp.where(eye, 2.0, 0.0) + value
            at = f * TILES + t
            second = f_high[at].astype(jnp.float32) + f_low[at].astype(jnp.float32)
            value = value + (second + made[t])
            value = value * inverses[place_of(f + offsets[at])][0:1]
            out_ref[f, t] = jnp.where(f < count, value, 0.0)

    for side in (0, 1):
        for k in range(6):
            copy(side, k).wait_send()


def shards(coupling, columns, row_slots):
    devices = lax.axis_size(AXIS)
    windows = [pltpu.VMEM((w, TILE, TILE), jnp.float32) for w in WIDTHS] * 4
    pool = pltpu.VMEM((ZERO + 1, TILE, TILE), jnp.bfloat16)
    anywhere = pl.BlockSpec(memory_space=pl.ANY)
    by_tile = columns.T
    return pl.pallas_call(
        functools.partial(kernel, devices),
        out_shape=jax.ShapeDtypeStruct(coupling.shape, coupling.dtype),
        in_specs=[anywhere, anywhere, pl.BlockSpec(memory_space=pltpu.SMEM)],
        out_specs=pl.BlockSpec(memory_space=pltpu.VMEM),
        scratch_shapes=[
            pltpu.VMEM(coupling.shape, jnp.float32),
            pltpu.SMEM(by_tile.shape, jnp.int32),
        ]
        + windows
        + [pool] * 4
        + [
            pltpu.VMEM((PLACES, 8, TILE), jnp.float32),
            pltpu.SMEM((PLACES * SPAN,), jnp.int32),
            pltpu.SMEM((10 * TILES,), jnp.int32),
            pltpu.SMEM((10 * NAMES,), jnp.int32),
            pltpu.SemaphoreType.DMA((2, 6)),
            pltpu.SemaphoreType.DMA((2, 6)),
            pltpu.SemaphoreType.DMA,
            pltpu.SemaphoreType.DMA,
        ],
        compiler_params=pltpu.CompilerParams(collective_id=0, has_side_effects=True),
        name="iterate",
    )(coupling, by_tile, row_slots)


def solution(mesh):
    return jax.shard_map(
        shards,
        mesh=mesh,
        in_specs=(P(AXIS, None, None, None), P(), P()),
        out_specs=P(AXIS, None, None, None),
        check_vma=False,
    )
```

```python
import functools

import jax
import jax.numpy as jnp
from jax import lax
from jax.experimental import pallas as pl
from jax.experimental.pallas import tpu as pltpu
from jax.sharding import PartitionSpec as P

TILE = 128
TILES = 5
SLOT = 4
BAND = 3
AXIS = "rows"
MESH = pl.DeviceIdType.MESH

WIDTHS = (5, 5, 5, 3, 2, 1)

WHOLE = 10 * TILES
PARTS = WIDTHS[3:]
ZERO = WHOLE + 2 * sum(PARTS)
PLACES = 16
SPAN = 2 * BAND + 1
NAMES = TILES * TILES


def first_row(slots_ref, bound):
    found = jnp.int32(0)
    step = slots_ref.shape[0] // 2
    while step:
        below = slots_ref[found + step - 1] < bound
        found = found + jnp.where(below, step, 0)
        step //= 2
    return found


def ownership(slots_ref, me):
    rows = slots_ref.shape[0]
    start = first_row(slots_ref, me * SLOT)
    count = jnp.int32(1)
    for k in range(1, SLOT):
        at = start + k
        inside = slots_ref[jnp.minimum(at, rows - 1)] < (me + 1) * SLOT
        count = count + jnp.where(jnp.logical_and(at < rows, inside), 1, 0)
    return start, count


def wrapped(value, rows):
    return lax.rem(value + rows, rows)


def signed(value, rows):
    half = rows // 2
    return lax.rem(value + rows + half, rows) - half


def inverse_column(tile, eye):
    return 1.0 / jnp.sum(jnp.where(eye, tile, 0.0), axis=1, keepdims=True)


def inverse_row(tile, eye):
    return 1.0 / jnp.sum(jnp.where(eye, tile, 0.0), axis=0, keepdims=True)


def split(value):
    high = value.astype(jnp.bfloat16)
    low = (value - high.astype(jnp.float32)).astype(jnp.bfloat16)
    return high, low


def dot(left, right):
    return jnp.dot(left, right, preferred_element_type=jnp.float32)


def multiply(left_high, left_low, base, pool_high, pool_low, names_ref, named):
    def block(pool, us, ts):
        return jnp.concatenate(
            [
                jnp.concatenate([pool[names_ref[named + u * TILES + t]] for t in ts], axis=1)
                for u in us
            ],
            axis=0,
        )

    def left(us):
        high = jnp.concatenate([left_high[base + u] for u in us], axis=1)
        low = jnp.concatenate([left_low[base + u] for u in us], axis=1)
        return high, jnp.concatenate([high, low], axis=0)

    pairs = ((0, 1), (2, 3))
    out = []
    for ts in pairs:
        total = None
        rest = None
        for us in pairs:
            high, both = left(us)
            part = dot(both, block(pool_high, us, ts))
            more = dot(high, block(pool_low, us, ts))
            total = part if total is None else total + part
            rest = more if rest is None else rest + more
        high = left_high[base + 4]
        low = left_low[base + 4]
        last = jnp.concatenate(
            [
                jnp.concatenate([high, high], axis=1),
                jnp.concatenate([low, jnp.zeros_like(low)], axis=1),
            ],
            axis=0,
        )
        right = jnp.concatenate([block(pool_high, (4,), ts), block(pool_low, (4,), ts)], axis=0)
        total = total + dot(last, right)
        value = total[:TILE] + total[TILE:] + rest
        out.append(value[:, :TILE])
        out.append(value[:, TILE:])
    total = None
    for us in pairs + ((4,),):
        right = jnp.concatenate([block(pool_high, us, (4,)), block(pool_low, us, (4,))], axis=1)
        part = dot(left(us)[1], right)
        total = part if total is None else total + part
    out.append(total[:TILE, :TILE] + (total[TILE:, :TILE] + total[:TILE, TILE:]))
    return out


def kernel(
    devices, own_hbm, columns_hbm, slots_hbm, out_ref, own_ref, columns_ref, slots_ref, *refs
):
    arriving = (refs[0:6], refs[6:12])
    leaving = (refs[12:18], refs[18:24])
    e_high, e_low, f_high, f_low, inverses, tiles, offsets, names = refs[24:32]
    send_sem, recv_sem, own_sem, columns_sem, slots_sem = refs[32:]
    rows = slots_ref.shape[0]
    me = lax.axis_index(AXIS)
    right, left = lax.rem(me + 1, devices), lax.rem(me + devices - 1, devices)
    odd = lax.rem(me, 2) == 1
    outward = jnp.where(odd, right, left)
    partner = jnp.where(odd, left, right)
    heading = (jnp.where(odd, 1, -1), jnp.where(odd, -1, 1))

    barrier = pltpu.get_barrier_semaphore()
    for other in (left, right):
        pl.semaphore_signal(barrier, inc=1, device_id=(other,), device_id_type=MESH)
    fetch_slots = pltpu.make_async_copy(slots_hbm, slots_ref, slots_sem)
    fetch_slots.start()
    fetch = pltpu.make_async_copy(own_hbm, own_ref, own_sem)
    fetch.start()
    fetch_columns = pltpu.make_async_copy(columns_hbm, columns_ref, columns_sem)
    fetch_columns.start()

    fetch_slots.wait()
    start, count = ownership(slots_ref, me)
    shape = (TILE, TILE)
    eye = lax.broadcasted_iota(jnp.int32, shape, 0) == lax.broadcasted_iota(jnp.int32, shape, 1)

    fetch.wait()
    pl.semaphore_wait(barrier, 2)

    def copy(side, k):
        return pltpu.make_async_remote_copy(
            src_ref=leaving[side][k],
            dst_ref=arriving[1 - side][k],
            send_sem=send_sem.at[side, k],
            recv_sem=recv_sem.at[1 - side, k],
            device_id=((outward, partner)[side],),
            device_id_type=MESH,
        )

    def await_row(side, k):
        copy(1 - side, k).wait_recv()

    def own_slot(side, k):
        return jnp.where(heading[side] > 0, jnp.maximum(count - 1 - k, 0), k)

    def fill_whole(side, k):
        received = arriving[side]
        target = leaving[side][k]
        for t in range(TILES):
            value = own_ref[own_slot(side, k), t]
            for held in range(1, k + 1):
                value = jnp.where(count == held, received[k - held][t], value)
            target[t] = value

    def tile_at_offset(row, offset):
        slot = slots_ref[row]
        target = wrapped(row + offset, rows)
        found = jnp.int32(0)
        for v in range(1, TILES):
            found = jnp.where(columns_ref[v, slot] == target, v, found)
        return found

    def fill_part(side, k):
        received = arriving[side]
        target = leaving[side][k]
        row = wrapped(jnp.where(heading[side] > 0, start + count - 1 - k, start + k), rows)
        whole = [(held, k - held) for held in range(1, SLOT + 1) if 0 <= k - held <= 2]
        diagonal = own_ref[own_slot(side, k), 0] if k == 3 else None
        for held, position in whole:
            tile = received[position][0]
            diagonal = tile if diagonal is None else jnp.where(count == held, tile, diagonal)
        scale = inverse_column(diagonal, eye)
        for place in range(WIDTHS[k]):
            offset = heading[side] * (BAND - WIDTHS[k] + 1 + place)
            index = tile_at_offset(row, offset)
            value = own_ref[own_slot(side, k), index] if k == 3 else None
            for held, position in whole:
                tile = received[position][index]
                value = tile if value is None else jnp.where(count == held, tile, value)
            value = jnp.where(index > 0, -(scale * value), 0.0)
            for held in range(1, SLOT + 1):
                position = k - held
                if position > 2:
                    ready = received[position][WIDTHS[position] - WIDTHS[k] + place]
                    value = jnp.where(count == held, ready, value)
            target[place] = value

    def forward(side, k):
        if k < 3:
            fill_whole(side, k)
        else:
            fill_part(side, k)
        copy(side, k).start()

    def distance(side, k):
        return jnp.where(heading[side] > 0, -1 - k, count + k)

    def place_of(d):
        below = jnp.where(odd, 6 + d, 9 - d)
        above = jnp.where(odd, 10 + d - count, 5 - d + count)
        return jnp.where(d < 0, below, jnp.where(d < count, 6 + d, above))

    def row_place(f):
        return 6 + f if f < 4 else (9 - f if f < 7 else 3 + f)

    def row_distance(f):
        return jnp.int32(f) if f < 4 else distance((f - 4) // 3, (f - 4) % 3)

    def convert_whole(f):
        source = own_ref.at[f] if f < 4 else arriving[(f - 4) // 3][(f - 4) % 3]
        diagonal = source[0]
        scale = inverse_column(diagonal, eye)
        inverses[row_place(f)] = jnp.broadcast_to(inverse_row(diagonal, eye), (8, TILE))
        for v in range(TILES):
            value = -(scale * source[v])
            if v == 0:
                value = jnp.where(eye, 1.0, 0.0) + value
            e_high[f * TILES + v], e_low[f * TILES + v] = split(value)

    def part_index(side, k):
        return WHOLE + side * sum(PARTS) + sum(PARTS[: k - 3])

    def convert_part(side, k):
        at = part_index(side, k)
        for n in range(WIDTHS[k]):
            e_high[at + n], e_low[at + n] = split(arriving[side][k][n])

    forward(0, 0)
    forward(1, 0)

    fetch_columns.wait()
    for f in range(10):
        row = wrapped(start + row_distance(f), rows)
        slot = slots_ref[row]
        found = [jnp.int32(ZERO)] * SPAN
        found[BAND] = jnp.int32(f * TILES)
        offsets[f * TILES] = 0
        for v in range(1, TILES):
            offset = jnp.clip(signed(columns_ref[v, slot] - row, rows), -BAND, BAND)
            offsets[f * TILES + v] = offset
            for o in range(SPAN):
                if o != BAND:
                    found[o] = jnp.where(offset == o - BAND, f * TILES + v, found[o])
        for o in range(SPAN):
            tiles[row_place(f) * SPAN + o] = found[o]
    for side in (0, 1):
        for k in range(3, 6):
            place = 5 - k if side == 0 else 10 + k
            for o in range(SPAN):
                tiles[place * SPAN + o] = ZERO
            for n in range(WIDTHS[k]):
                offset = heading[side] * (BAND - WIDTHS[k] + 1 + n)
                tiles[place * SPAN + BAND + offset] = part_index(side, k) + n

    @pl.loop(0, 10)
    def _(f):
        stream = jnp.where(f < 7, heading[0], heading[1])
        k = jnp.where(f < 7, f - 4, f - 7)
        d = jnp.where(f < 4, f, jnp.where(stream > 0, -1 - k, count + k))
        for u in range(TILES):
            first = offsets[f * TILES + u]
            place = place_of(d + first)
            for t in range(TILES):
                offset = offsets[f * TILES + t] - first
                near = jnp.logical_and(offset <= BAND, offset >= -BAND)
                at = place * SPAN + BAND + jnp.where(near, offset, 0)
                names[f * NAMES + u * TILES + t] = jnp.where(near, tiles[at], ZERO)

    zeros = jnp.zeros((TILE, TILE), jnp.bfloat16)
    for pool in (e_high, e_low, f_high, f_low):
        pool[ZERO] = zeros
    for f in range(4):
        convert_whole(f)

    for k in range(1, 4):
        for side in (0, 1):
            await_row(side, k - 1)
            forward(side, k)
            convert_whole(4 + 3 * side + k - 1)

    def square(f):
        made = multiply(e_high, e_low, f * TILES, e_high, e_low, names, f * NAMES)
        for t in range(TILES):
            f_high[f * TILES + t], f_low[f * TILES + t] = split(made[t])

    pl.loop(0, 2)(square)
    for k in (4, 5):
        for side in (0, 1):
            await_row(side, k - 1)
            forward(side, k)
            convert_part(side, k - 1)
        if k == 4:
            pl.loop(2, 4)(square)
        pl.loop(0, 2)(lambda side: square(4 + 3 * side + (k - 4)))
    for side in (0, 1):
        await_row(side, 5)
        convert_part(side, 5)
    pl.loop(0, 2)(lambda side: square(4 + 3 * side + 2))

    @pl.loop(0, SLOT)
    def _(f):
        made = multiply(e_high, e_low, f * TILES, f_high, f_low, names, f * NAMES)
        scale = inverse_column(own_ref[f, 0], eye)
        for t in range(TILES):
            value = -(scale * own_ref[f, t])
            if t == 0:
                value = jnp.where(eye, 2.0, 0.0) + value
            at = f * TILES + t
            second = f_high[at].astype(jnp.float32) + f_low[at].astype(jnp.float32)
            value = value + (second + made[t])
            value = value * inverses[place_of(f + offsets[at])][0:1]
            out_ref[f, t] = jnp.where(f < count, value, 0.0)

    for side in (0, 1):
        for k in range(6):
            copy(side, k).wait_send()


def shards(coupling, columns, row_slots):
    devices = lax.axis_size(AXIS)
    windows = [pltpu.VMEM((w, TILE, TILE), jnp.float32) for w in WIDTHS] * 4
    pool = pltpu.VMEM((ZERO + 1, TILE, TILE), jnp.bfloat16)
    anywhere = pl.BlockSpec(memory_space=pl.ANY)
    by_tile = columns.T
    return pl.pallas_call(
        functools.partial(kernel, devices),
        out_shape=pltpu.VMEM(coupling.shape, coupling.dtype),
        in_specs=[anywhere] * 3,
        out_specs=pl.BlockSpec(memory_space=pltpu.VMEM),
        scratch_shapes=[
            pltpu.VMEM(coupling.shape, jnp.float32),
            pltpu.SMEM(by_tile.shape, jnp.int32),
            pltpu.SMEM(row_slots.shape, jnp.int32),
        ]
        + windows
        + [pool] * 4
        + [
            pltpu.VMEM((PLACES, 8, TILE), jnp.float32),
            pltpu.SMEM((PLACES * SPAN,), jnp.int32),
            pltpu.SMEM((10 * TILES,), jnp.int32),
            pltpu.SMEM((10 * NAMES,), jnp.int32),
            pltpu.SemaphoreType.DMA((2, 6)),
            pltpu.SemaphoreType.DMA((2, 6)),
            pltpu.SemaphoreType.DMA,
            pltpu.SemaphoreType.DMA,
            pltpu.SemaphoreType.DMA,
        ],
        compiler_params=pltpu.CompilerParams(collective_id=0, has_side_effects=True),
        name="iterate",
    )(coupling, by_tile, row_slots)


def solution(mesh):
    return jax.shard_map(
        shards,
        mesh=mesh,
        in_specs=(P(AXIS, None, None, None), P(), P()),
        out_specs=P(AXIS, None, None, None),
        check_vma=False,
    )
```

```python
import functools

import jax
import jax.numpy as jnp
from jax import lax
from jax.experimental import pallas as pl
from jax.experimental.pallas import tpu as pltpu
from jax.sharding import PartitionSpec as P

TILE = 128
TILES = 5
SLOT = 4
BAND = 3
AXIS = "rows"
MESH = pl.DeviceIdType.MESH

WIDTHS = (5, 5, 5, 3, 2, 1)

WHOLE = 14 * TILES
PARTS = WIDTHS[3:]
ZERO = WHOLE + 2 * sum(PARTS)
SOURCES = 20
F_ROWS = 10
F_ZERO = F_ROWS * TILES
SPAN = 2 * BAND + 1
NAMES = TILES * TILES


def first_row(slots_ref, bound):
    found = jnp.int32(0)
    step = slots_ref.shape[0] // 2
    while step:
        below = slots_ref[found + step - 1] < bound
        found = found + jnp.where(below, step, 0)
        step //= 2
    return found


def held(slots_ref, start, device):
    rows = slots_ref.shape[0]
    count = jnp.int32(1)
    for k in range(1, SLOT):
        at = start + k
        inside = slots_ref[jnp.minimum(at, rows - 1)] < (device + 1) * SLOT
        count = count + jnp.where(jnp.logical_and(at < rows, inside), 1, 0)
    return count


def wrapped(value, rows):
    return lax.rem(value + rows, rows)


def signed(value, rows):
    half = rows // 2
    return lax.rem(value + rows + half, rows) - half


def inverse_column(tile, eye):
    return 1.0 / jnp.sum(jnp.where(eye, tile, 0.0), axis=1, keepdims=True)


def inverse_row(tile, eye):
    return 1.0 / jnp.sum(jnp.where(eye, tile, 0.0), axis=0, keepdims=True)


def split(value):
    high = value.astype(jnp.bfloat16)
    low = (value - high.astype(jnp.float32)).astype(jnp.bfloat16)
    return high, low


def dot(left, right):
    return jnp.dot(left, right, preferred_element_type=jnp.float32)


def multiply(left_high, left_low, base, pool_high, pool_low, names_ref, named):
    def block(pool, us, ts):
        return jnp.concatenate(
            [
                jnp.concatenate([pool[names_ref[named + u * TILES + t]] for t in ts], axis=1)
                for u in us
            ],
            axis=0,
        )

    def left(us):
        high = jnp.concatenate([left_high[base + u] for u in us], axis=1)
        low = jnp.concatenate([left_low[base + u] for u in us], axis=1)
        return high, jnp.concatenate([high, low], axis=0)

    pairs = ((0, 1), (2, 3))
    out = []
    for ts in pairs:
        total = None
        rest = None
        for us in pairs:
            high, both = left(us)
            part = dot(both, block(pool_high, us, ts))
            more = dot(high, block(pool_low, us, ts))
            total = part if total is None else total + part
            rest = more if rest is None else rest + more
        high = left_high[base + 4]
        low = left_low[base + 4]
        last = jnp.concatenate(
            [
                jnp.concatenate([high, high], axis=1),
                jnp.concatenate([low, jnp.zeros_like(low)], axis=1),
            ],
            axis=0,
        )
        right = jnp.concatenate([block(pool_high, (4,), ts), block(pool_low, (4,), ts)], axis=0)
        total = total + dot(last, right)
        value = total[:TILE] + total[TILE:] + rest
        out.append(value[:, :TILE])
        out.append(value[:, TILE:])
    total = None
    for us in pairs + ((4,),):
        right = jnp.concatenate([block(pool_high, us, (4,)), block(pool_low, us, (4,))], axis=1)
        part = dot(left(us)[1], right)
        total = part if total is None else total + part
    out.append(total[:TILE, :TILE] + (total[TILE:, :TILE] + total[:TILE, TILE:]))
    return out


def kernel(
    devices,
    own_hbm,
    columns_hbm,
    slots_hbm,
    out_ref,
    own_ref,
    partner_ref,
    columns_ref,
    slots_ref,
    *refs,
):
    leaving, arriving, passed = refs[0:6], refs[6:12], refs[12:18]
    e_high, e_low, f_high, f_low, inverses = refs[18:23]
    tiles, offsets, bases, names, f_names = refs[23:28]
    out_send, out_recv, pass_send, pass_recv, row_send, row_recv = refs[28:34]
    own_sem, columns_sem, slots_sem = refs[34:]
    rows = slots_ref.shape[0]
    me = lax.axis_index(AXIS)
    parity = lax.rem(me, 2)
    odd = parity == 1
    above, below = lax.rem(me + 2, devices), lax.rem(me + devices - 2, devices)
    outward = jnp.where(odd, above, below)
    partner = me + 1 - 2 * parity
    heading = 2 * parity - 1

    barrier = pltpu.get_barrier_semaphore()
    for other in (above, below, partner):
        pl.semaphore_signal(barrier, inc=1, device_id=(other,), device_id_type=MESH)
    fetch_slots = pltpu.make_async_copy(slots_hbm, slots_ref, slots_sem)
    fetch_slots.start()
    fetch = pltpu.make_async_copy(own_hbm, own_ref, own_sem)
    fetch.start()
    fetch_columns = pltpu.make_async_copy(columns_hbm, columns_ref, columns_sem)
    fetch_columns.start()

    shape = (TILE, TILE)
    eye = lax.broadcasted_iota(jnp.int32, shape, 0) == lax.broadcasted_iota(jnp.int32, shape, 1)

    fetch_slots.wait()
    chip_start = first_row(slots_ref, (me - parity) * SLOT)
    low_count = held(slots_ref, chip_start, me - parity)
    middle = chip_start + low_count
    high_count = held(slots_ref, middle, me - parity + 1)
    chip_end = middle + high_count
    start = jnp.where(odd, middle, chip_start)
    count = jnp.where(odd, high_count, low_count)
    partner_count = jnp.where(odd, low_count, high_count)
    partner_start = jnp.where(odd, chip_start, middle)

    fetch.wait()
    pl.semaphore_wait(barrier, 3)

    def remote(source, target, send, recv, device):
        return pltpu.make_async_remote_copy(
            src_ref=source,
            dst_ref=target,
            send_sem=send,
            recv_sem=recv,
            device_id=(device,),
            device_id_type=MESH,
        )

    def send_out(k):
        return remote(leaving[k], arriving[k], out_send.at[k], out_recv.at[k], outward)

    def pass_on(k):
        return remote(arriving[k], passed[k], pass_send.at[k], pass_recv.at[k], partner)

    share = remote(own_ref, partner_ref, row_send, row_recv, partner)

    def row_of(source):
        if source < 4:
            row = start + source
        elif source < 8:
            row = partner_start + (source - 4)
        elif source < 14:
            k = source - 8
            row = jnp.where(odd, chip_start - 1 - k, chip_end + k)
        else:
            k = source - 14
            row = jnp.where(odd, chip_end + k, chip_start - 1 - k)
        return wrapped(row, rows)

    def whole_row(source):
        return jnp.where(source < 11, source, source - 3)

    def source_of(m):
        inner = -1 - m
        beyond = 8 + inner - partner_count
        beside = 4 + jnp.where(odd, partner_count - 1 - inner, inner)
        own = jnp.where(odd, m, count - 1 - m)
        outer = 14 + m - count
        near = jnp.where(inner < partner_count, beside, beyond)
        source = jnp.where(m < 0, near, jnp.where(m < count, own, outer))
        return jnp.clip(source, 0, SOURCES - 1)

    def f_row_of(m):
        own = jnp.where(odd, m, count - 1 - m)
        row = jnp.where(m < 0, 3 - m, jnp.where(m < count, own, 7 + m - count))
        return jnp.clip(row, 0, F_ROWS - 1)

    def own_slot(k):
        return jnp.where(odd, jnp.maximum(count - 1 - k, 0), k)

    def partner_slot(inner):
        return jnp.clip(jnp.where(odd, partner_count - 1 - inner, inner), 0, SLOT - 1)

    def fill_whole(k):
        inner = k - count
        for t in range(TILES):
            value = own_ref[own_slot(k), t]
            if k > 0:
                value = jnp.where(inner >= 0, partner_ref[partner_slot(inner), t], value)
            for j in range(k - 1):
                value = jnp.where(inner - partner_count == j, arriving[j][t], value)
            leaving[k][t] = value

    def tile_at_offset(row, offset):
        slot = slots_ref[row]
        target = wrapped(row + offset, rows)
        found = jnp.int32(0)
        for v in range(1, TILES):
            found = jnp.where(columns_ref[v, slot] == target, v, found)
        return found

    def fill_part(k):
        inner = k - count
        beyond = inner - partner_count
        row = wrapped(jnp.where(odd, chip_end - 1 - k, chip_start + k), rows)

        def pick(t):
            value = partner_ref[partner_slot(inner), t]
            if k < SLOT:
                value = jnp.where(inner < 0, own_ref[own_slot(k), t], value)
            for j in range(min(k - 1, 3)):
                value = jnp.where(beyond == j, arriving[j][t], value)
            return value

        scale = inverse_column(pick(0), eye)
        for place in range(WIDTHS[k]):
            offset = heading * (BAND - WIDTHS[k] + 1 + place)
            index = tile_at_offset(row, offset)
            value = jnp.where(index > 0, -(scale * pick(index)), 0.0)
            for j in range(3, k - 1):
                ready = arriving[j][WIDTHS[j] - WIDTHS[k] + place]
                value = jnp.where(beyond == j, ready, value)
            leaving[k][place] = value

    def forward(k):
        if k < 3:
            fill_whole(k)
        else:
            fill_part(k)
        send_out(k).start()

    def convert_whole(e):
        if e < 4:
            source = own_ref.at[e]
        elif e < 8:
            source = partner_ref.at[e - 4]
        else:
            source = arriving[e - 8] if e < 11 else passed[e - 11]
        diagonal = source[0]
        scale = inverse_column(diagonal, eye)
        inverses[e] = jnp.broadcast_to(inverse_row(diagonal, eye), (8, TILE))
        for v in range(TILES):
            value = -(scale * source[v])
            if v == 0:
                value = jnp.where(eye, 1.0, 0.0) + value
            e_high[e * TILES + v], e_low[e * TILES + v] = split(value)

    def part_index(side, k):
        return WHOLE + side * sum(PARTS) + sum(PARTS[: k - 3])

    def convert_part(side, k):
        at = part_index(side, k)
        for n in range(WIDTHS[k]):
            e_high[at + n], e_low[at + n] = split((arriving, passed)[side][k][n])

    forward(0)
    share.start()

    fetch_columns.wait()
    for e in range(14):
        source = e if e < 11 else e + 3
        row = row_of(source)
        slot = slots_ref[row]
        found = [jnp.int32(ZERO)] * SPAN
        found[BAND] = jnp.int32(e * TILES)
        offsets[e * TILES] = 0
        for v in range(1, TILES):
            offset = jnp.clip(signed(columns_ref[v, slot] - row, rows), -BAND, BAND)
            offsets[e * TILES + v] = offset
            for o in range(SPAN):
                if o != BAND:
                    found[o] = jnp.where(offset == o - BAND, e * TILES + v, found[o])
        for o in range(SPAN):
            tiles[source * SPAN + o] = found[o]
    for side in (0, 1):
        for k in range(3, 6):
            source = 8 + 6 * side + k
            for o in range(SPAN):
                tiles[source * SPAN + o] = ZERO
            for n in range(WIDTHS[k]):
                offset = heading * (1 - 2 * side) * (BAND - WIDTHS[k] + 1 + n)
                tiles[source * SPAN + BAND + offset] = part_index(side, k) + n

    zeros = jnp.zeros((TILE, TILE), jnp.bfloat16)
    e_high[ZERO] = zeros
    e_low[ZERO] = zeros
    f_high[F_ZERO] = zeros
    f_low[F_ZERO] = zeros
    for e in range(4):
        convert_whole(e)

    share.wait_recv()
    forward(1)

    def distance(f):
        own = jnp.where(odd, f, count - 1 - f)
        return jnp.where(f < 4, own, jnp.where(f < 7, 3 - f, count + f - 7))

    @pl.loop(0, F_ROWS)
    def _(f):
        m = distance(f)
        source = jnp.where(f < 4, f, source_of(m))
        base = whole_row(source) * TILES
        bases[f] = base
        for u in range(TILES):
            first = offsets[base + u]
            at = source_of(m + heading * first)
            shift = f_row_of(m + heading * first) * TILES - whole_row(at) * TILES
            for t in range(TILES):
                offset = offsets[base + t] - first
                near = jnp.logical_and(offset <= BAND, offset >= -BAND)
                name = tiles[at * SPAN + BAND + jnp.where(near, offset, 0)]
                name = jnp.where(near, name, ZERO)
                names[f * NAMES + u * TILES + t] = name
                moved = jnp.clip(name + shift, 0, F_ZERO - 1)
                f_names[f * NAMES + u * TILES + t] = jnp.where(name == ZERO, F_ZERO, moved)

    for e in range(4, 8):
        convert_whole(e)

    def square(f):
        made = multiply(e_high, e_low, bases[f], e_high, e_low, names, f * NAMES)
        for t in range(TILES):
            f_high[f * TILES + t], f_low[f * TILES + t] = split(made[t])

    def receive(k):
        send_out(k).wait_recv()
        pass_on(k).start()

    def take(k):
        pass_on(k).wait_recv()
        if k < 3:
            convert_whole(11 + k)
        else:
            convert_part(1, k)

    for k in range(2, 6):
        receive(k - 2)
        forward(k)
        if k < 5:
            convert_whole(6 + k)
        else:
            convert_part(0, 3)
        if k > 2:
            take(k - 3)
    pl.loop(0, 4)(square)
    take(3)
    pl.loop(7, 8)(square)
    receive(4)
    convert_part(0, 4)
    pl.loop(4, 6)(square)
    take(4)
    pl.loop(8, 9)(square)
    receive(5)
    pl.loop(6, 7)(square)
    take(5)
    pl.loop(9, 10)(square)

    @pl.loop(0, SLOT)
    def _(f):
        made = multiply(e_high, e_low, f * TILES, f_high, f_low, f_names, f * NAMES)
        scale = inverse_column(own_ref[f, 0], eye)
        m = distance(f)
        for t in range(TILES):
            value = -(scale * own_ref[f, t])
            if t == 0:
                value = jnp.where(eye, 2.0, 0.0) + value
            at = f * TILES + t
            second = f_high[at].astype(jnp.float32) + f_low[at].astype(jnp.float32)
            value = value + (second + made[t])
            column = whole_row(source_of(m + heading * offsets[at]))
            value = value * inverses[jnp.minimum(column, 13)][0:1]
            out_ref[f, t] = jnp.where(f < count, value, 0.0)

    share.wait_send()
    for k in range(6):
        send_out(k).wait_send()
        pass_on(k).wait_send()


def shards(coupling, columns, row_slots):
    devices = lax.axis_size(AXIS)
    windows = [pltpu.VMEM((w, TILE, TILE), jnp.float32) for w in WIDTHS] * 3
    e_pool = pltpu.VMEM((ZERO + 1, TILE, TILE), jnp.bfloat16)
    f_pool = pltpu.VMEM((F_ZERO + 1, TILE, TILE), jnp.bfloat16)
    anywhere = pl.BlockSpec(memory_space=pl.ANY)
    by_tile = columns.T
    semaphore = pltpu.SemaphoreType.DMA
    return pl.pallas_call(
        functools.partial(kernel, devices),
        out_shape=pltpu.VMEM(coupling.shape, coupling.dtype),
        in_specs=[anywhere] * 3,
        out_specs=pl.BlockSpec(memory_space=pltpu.VMEM),
        scratch_shapes=[
            pltpu.VMEM(coupling.shape, jnp.float32),
            pltpu.VMEM(coupling.shape, jnp.float32),
            pltpu.SMEM(by_tile.shape, jnp.int32),
            pltpu.SMEM(row_slots.shape, jnp.int32),
        ]
        + windows
        + [e_pool, e_pool, f_pool, f_pool]
        + [
            pltpu.VMEM((14, 8, TILE), jnp.float32),
            pltpu.SMEM((SOURCES * SPAN,), jnp.int32),
            pltpu.SMEM((14 * TILES,), jnp.int32),
            pltpu.SMEM((F_ROWS,), jnp.int32),
            pltpu.SMEM((F_ROWS * NAMES,), jnp.int32),
            pltpu.SMEM((F_ROWS * NAMES,), jnp.int32),
        ]
        + [semaphore((6,))] * 4
        + [semaphore] * 5,
        compiler_params=pltpu.CompilerParams(collective_id=0, has_side_effects=True),
        name="iterate",
    )(coupling, by_tile, row_slots)


def solution(mesh):
    return jax.shard_map(
        shards,
        mesh=mesh,
        in_specs=(P(AXIS, None, None, None), P(), P()),
        out_specs=P(AXIS, None, None, None),
        check_vma=False,
    )
```

```python
import functools

import jax
import jax.numpy as jnp
from jax import lax
from jax.experimental import pallas as pl
from jax.experimental.pallas import tpu as pltpu
from jax.sharding import PartitionSpec as P

TILE = 128
TILES = 5
SLOT = 4
BAND = 3
AXIS = "rows"
RUN = 128
MESH = pl.DeviceIdType.MESH

WIDTHS = (5, 5, 5, 3, 2, 1)

WHOLE = 14 * TILES
PARTS = WIDTHS[3:]
ZERO = WHOLE + 2 * sum(PARTS)
SOURCES = 20
F_ROWS = 10
F_ZERO = F_ROWS * TILES
SPAN = 2 * BAND + 1
NAMES = TILES * TILES


def first_row(slots_ref, bound):
    found = jnp.int32(0)
    step = slots_ref.shape[0] // 2
    while step:
        below = slots_ref[found + step - 1] < bound
        found = found + jnp.where(below, step, 0)
        step //= 2
    return found


def held(slots_ref, start, device):
    rows = slots_ref.shape[0]
    count = jnp.int32(1)
    for k in range(1, SLOT):
        at = start + k
        inside = slots_ref[jnp.minimum(at, rows - 1)] < (device + 1) * SLOT
        count = count + jnp.where(jnp.logical_and(at < rows, inside), 1, 0)
    return count


def wrapped(value, rows):
    return lax.rem(value + rows, rows)


def signed(value, rows):
    half = rows // 2
    return lax.rem(value + rows + half, rows) - half


def inverse_column(tile, eye):
    return 1.0 / jnp.sum(jnp.where(eye, tile, 0.0), axis=1, keepdims=True)


def inverse_row(tile, eye):
    return 1.0 / jnp.sum(jnp.where(eye, tile, 0.0), axis=0, keepdims=True)


def split(value):
    high = value.astype(jnp.bfloat16)
    low = (value - high.astype(jnp.float32)).astype(jnp.bfloat16)
    return high, low


def dot(left, right):
    return jnp.dot(left, right, preferred_element_type=jnp.float32)


def multiply(left_high, left_low, base, pool_high, pool_low, names_ref, named):
    def block(pool, us, ts):
        return jnp.concatenate(
            [
                jnp.concatenate([pool[names_ref[named + u * TILES + t]] for t in ts], axis=1)
                for u in us
            ],
            axis=0,
        )

    def left(us):
        high = jnp.concatenate([left_high[base + u] for u in us], axis=1)
        low = jnp.concatenate([left_low[base + u] for u in us], axis=1)
        return high, jnp.concatenate([high, low], axis=0)

    pairs = ((0, 1), (2, 3))
    out = []
    for ts in pairs:
        total = None
        rest = None
        for us in pairs:
            high, both = left(us)
            part = dot(both, block(pool_high, us, ts))
            more = dot(high, block(pool_low, us, ts))
            total = part if total is None else total + part
            rest = more if rest is None else rest + more
        high = left_high[base + 4]
        low = left_low[base + 4]
        last = jnp.concatenate(
            [
                jnp.concatenate([high, high], axis=1),
                jnp.concatenate([low, jnp.zeros_like(low)], axis=1),
            ],
            axis=0,
        )
        right = jnp.concatenate([block(pool_high, (4,), ts), block(pool_low, (4,), ts)], axis=0)
        total = total + dot(last, right)
        value = total[:TILE] + total[TILE:] + rest
        out.append(value[:, :TILE])
        out.append(value[:, TILE:])
    total = None
    for us in pairs + ((4,),):
        right = jnp.concatenate([block(pool_high, us, (4,)), block(pool_low, us, (4,))], axis=1)
        part = dot(left(us)[1], right)
        total = part if total is None else total + part
    out.append(total[:TILE, :TILE] + (total[TILE:, :TILE] + total[:TILE, TILE:]))
    return out


def kernel(
    devices,
    own_hbm,
    columns_hbm,
    slots_hbm,
    out_ref,
    own_ref,
    partner_ref,
    columns_ref,
    slots_ref,
    *refs,
):
    leaving, arriving, passed = refs[0:6], refs[6:12], refs[12:18]
    e_high, e_low, f_high, f_low, inverses = refs[18:23]
    tiles, offsets, bases, names, f_names = refs[23:28]
    out_send, out_recv, pass_send, pass_recv, row_send, row_recv = refs[28:34]
    own_sem, columns_sem, slots_sem = refs[34:]
    rows = slots_ref.shape[0]
    me = lax.axis_index(AXIS)
    parity = lax.rem(me, 2)
    odd = parity == 1
    above, below = lax.rem(me + 2, devices), lax.rem(me + devices - 2, devices)
    outward = jnp.where(odd, above, below)
    partner = me + 1 - 2 * parity
    heading = 2 * parity - 1

    barrier = pltpu.get_barrier_semaphore()
    for other in (above, below, partner):
        pl.semaphore_signal(barrier, inc=1, device_id=(other,), device_id_type=MESH)
    fetch_slots = pltpu.make_async_copy(slots_hbm, slots_ref, slots_sem)
    fetch_slots.start()
    fetch = pltpu.make_async_copy(own_hbm, own_ref, own_sem)
    fetch.start()
    fetch_columns = pltpu.make_async_copy(columns_hbm, columns_ref, columns_sem)
    fetch_columns.start()

    shape = (TILE, TILE)
    eye = lax.broadcasted_iota(jnp.int32, shape, 0) == lax.broadcasted_iota(jnp.int32, shape, 1)

    fetch_slots.wait()
    chip_start = first_row(slots_ref, (me - parity) * SLOT)
    low_count = held(slots_ref, chip_start, me - parity)
    middle = chip_start + low_count
    high_count = held(slots_ref, middle, me - parity + 1)
    chip_end = middle + high_count
    start = jnp.where(odd, middle, chip_start)
    count = jnp.where(odd, high_count, low_count)
    partner_count = jnp.where(odd, low_count, high_count)
    partner_start = jnp.where(odd, chip_start, middle)


    def remote(source, target, send, recv, device):
        return pltpu.make_async_remote_copy(
            src_ref=source,
            dst_ref=target,
            send_sem=send,
            recv_sem=recv,
            device_id=(device,),
            device_id_type=MESH,
        )

    def send_out(k):
        return remote(leaving[k], arriving[k], out_send.at[k], out_recv.at[k], outward)

    def pass_on(k):
        return remote(arriving[k], passed[k], pass_send.at[k], pass_recv.at[k], partner)

    share = remote(own_ref, partner_ref, row_send, row_recv, partner)

    def row_of(source):
        if source < 4:
            row = start + source
        elif source < 8:
            row = partner_start + (source - 4)
        elif source < 14:
            k = source - 8
            row = jnp.where(odd, chip_start - 1 - k, chip_end + k)
        else:
            k = source - 14
            row = jnp.where(odd, chip_end + k, chip_start - 1 - k)
        return wrapped(row, rows)

    def whole_row(source):
        return jnp.where(source < 11, source, source - 3)

    def source_of(m):
        inner = -1 - m
        beyond = 8 + inner - partner_count
        beside = 4 + jnp.where(odd, partner_count - 1 - inner, inner)
        own = jnp.where(odd, m, count - 1 - m)
        outer = 14 + m - count
        near = jnp.where(inner < partner_count, beside, beyond)
        source = jnp.where(m < 0, near, jnp.where(m < count, own, outer))
        return jnp.clip(source, 0, SOURCES - 1)

    def f_row_of(m):
        own = jnp.where(odd, m, count - 1 - m)
        row = jnp.where(m < 0, 3 - m, jnp.where(m < count, own, 7 + m - count))
        return jnp.clip(row, 0, F_ROWS - 1)

    def own_slot(k):
        return jnp.where(odd, jnp.maximum(count - 1 - k, 0), k)

    def partner_slot(inner):
        return jnp.clip(jnp.where(odd, partner_count - 1 - inner, inner), 0, SLOT - 1)

    def fill_whole(k):
        inner = k - count
        for t in range(TILES):
            value = own_ref[own_slot(k), t]
            if k > 0:
                value = jnp.where(inner >= 0, partner_ref[partner_slot(inner), t], value)
            for j in range(k - 1):
                value = jnp.where(inner - partner_count == j, arriving[j][t], value)
            leaving[k][t] = value

    def tile_at_offset(row, offset):
        slot = slots_ref[row]
        target = wrapped(row + offset, rows)
        found = jnp.int32(0)
        for v in range(1, TILES):
            found = jnp.where(columns_ref[v, slot] == target, v, found)
        return found

    def fill_part(k):
        inner = k - count
        beyond = inner - partner_count
        row = wrapped(jnp.where(odd, chip_end - 1 - k, chip_start + k), rows)

        def pick(t):
            value = partner_ref[partner_slot(inner), t]
            if k < SLOT:
                value = jnp.where(inner < 0, own_ref[own_slot(k), t], value)
            for j in range(min(k - 1, 3)):
                value = jnp.where(beyond == j, arriving[j][t], value)
            return value

        scale = inverse_column(pick(0), eye)
        for place in range(WIDTHS[k]):
            offset = heading * (BAND - WIDTHS[k] + 1 + place)
            index = tile_at_offset(row, offset)
            value = jnp.where(index > 0, -(scale * pick(index)), 0.0)
            for j in range(3, k - 1):
                ready = arriving[j][WIDTHS[j] - WIDTHS[k] + place]
                value = jnp.where(beyond == j, ready, value)
            leaving[k][place] = value

    def forward(k):
        if k < 3:
            fill_whole(k)
        else:
            fill_part(k)
        send_out(k).start()

    def convert_whole(e):
        if e < 4:
            source = own_ref.at[e]
        elif e < 8:
            source = partner_ref.at[e - 4]
        else:
            source = arriving[e - 8] if e < 11 else passed[e - 11]
        diagonal = source[0]
        scale = inverse_column(diagonal, eye)
        inverses[e] = jnp.broadcast_to(inverse_row(diagonal, eye), (8, TILE))
        for v in range(TILES):
            value = -(scale * source[v])
            if v == 0:
                value = jnp.where(eye, 1.0, 0.0) + value
            e_high[e * TILES + v], e_low[e * TILES + v] = split(value)

    def part_index(side, k):
        return WHOLE + side * sum(PARTS) + sum(PARTS[: k - 3])

    def convert_part(side, k):
        at = part_index(side, k)
        for n in range(WIDTHS[k]):
            e_high[at + n], e_low[at + n] = split((arriving, passed)[side][k][n])

    fetch.wait()
    fill_whole(0)
    pl.semaphore_wait(barrier, 3)
    send_out(0).start()
    share.start()

    fetch_columns.wait()
    for e in range(14):
        source = e if e < 11 else e + 3
        row = row_of(source)
        slot = slots_ref[row]
        found = [jnp.int32(ZERO)] * SPAN
        found[BAND] = jnp.int32(e * TILES)
        offsets[e * TILES] = 0
        for v in range(1, TILES):
            offset = jnp.clip(signed(columns_ref[v, slot] - row, rows), -BAND, BAND)
            offsets[e * TILES + v] = offset
            for o in range(SPAN):
                if o != BAND:
                    found[o] = jnp.where(offset == o - BAND, e * TILES + v, found[o])
        for o in range(SPAN):
            tiles[source * SPAN + o] = found[o]
    for side in (0, 1):
        for k in range(3, 6):
            source = 8 + 6 * side + k
            for o in range(SPAN):
                tiles[source * SPAN + o] = ZERO
            for n in range(WIDTHS[k]):
                offset = heading * (1 - 2 * side) * (BAND - WIDTHS[k] + 1 + n)
                tiles[source * SPAN + BAND + offset] = part_index(side, k) + n

    zeros = jnp.zeros((TILE, TILE), jnp.bfloat16)
    e_high[ZERO] = zeros
    e_low[ZERO] = zeros
    f_high[F_ZERO] = zeros
    f_low[F_ZERO] = zeros
    for e in range(4):
        convert_whole(e)

    share.wait_recv()
    forward(1)

    def distance(f):
        own = jnp.where(odd, f, count - 1 - f)
        return jnp.where(f < 4, own, jnp.where(f < 7, 3 - f, count + f - 7))

    @pl.loop(0, F_ROWS)
    def _(f):
        m = distance(f)
        source = jnp.where(f < 4, f, source_of(m))
        base = whole_row(source) * TILES
        bases[f] = base
        for u in range(TILES):
            first = offsets[base + u]
            at = source_of(m + heading * first)
            shift = f_row_of(m + heading * first) * TILES - whole_row(at) * TILES
            for t in range(TILES):
                offset = offsets[base + t] - first
                near = jnp.logical_and(offset <= BAND, offset >= -BAND)
                name = tiles[at * SPAN + BAND + jnp.where(near, offset, 0)]
                name = jnp.where(near, name, ZERO)
                names[f * NAMES + u * TILES + t] = name
                moved = jnp.clip(name + shift, 0, F_ZERO - 1)
                f_names[f * NAMES + u * TILES + t] = jnp.where(name == ZERO, F_ZERO, moved)

    for e in range(4, 8):
        convert_whole(e)

    def square(f):
        made = multiply(e_high, e_low, bases[f], e_high, e_low, names, f * NAMES)
        for t in range(TILES):
            f_high[f * TILES + t], f_low[f * TILES + t] = split(made[t])

    def receive(k):
        send_out(k).wait_recv()
        pass_on(k).start()

    def take(k):
        pass_on(k).wait_recv()
        if k < 3:
            convert_whole(11 + k)
        else:
            convert_part(1, k)

    place = lax.rem(me, RUN)
    late_up = place == 1
    late_passed = place == 0

    def squares(first, last):
        pl.loop(first, last)(square)

    def choose(up, other):
        return jnp.where(late_up, up, other)

    @pl.when(late_up)
    def _():
        for k in range(6):
            take(k)

    squares(8, choose(10, 8))
    for k in range(2, 6):
        receive(k - 2)
        forward(k)
        if k < 5:
            convert_whole(6 + k)
        else:
            convert_part(0, 3)
        if k > 2:

            @pl.when(place > 1)
            def _():
                take(k - 3)

        if k == 4:
            squares(0, choose(5, 0))

    @pl.when(late_passed)
    def _():
        receive(4)
        convert_part(0, 4)
        receive(5)

    squares(6, jnp.where(late_passed, 7, 6))

    @pl.when(late_passed)
    def _():
        for k in range(3):
            take(k)

    squares(choose(5, 0), choose(6, 4))

    def take_unless_taken(k):
        @pl.when(jnp.logical_not(late_up))
        def _():
            take(k)

    take_unless_taken(3)
    squares(7, 8)

    @pl.when(jnp.logical_not(late_passed))
    def _():
        receive(4)
        convert_part(0, 4)

    squares(choose(6, 4), 6)
    take_unless_taken(4)
    squares(choose(9, 8), 9)
    squares(jnp.where(late_passed, 7, 6), 7)

    @pl.when(jnp.logical_not(late_passed))
    def _():
        receive(5)

    take_unless_taken(5)
    squares(choose(10, 9), 10)

    @pl.loop(0, SLOT)
    def _(f):
        made = multiply(e_high, e_low, f * TILES, f_high, f_low, f_names, f * NAMES)
        scale = inverse_column(own_ref[f, 0], eye)
        m = distance(f)
        for t in range(TILES):
            value = -(scale * own_ref[f, t])
            if t == 0:
                value = jnp.where(eye, 2.0, 0.0) + value
            at = f * TILES + t
            second = f_high[at].astype(jnp.float32) + f_low[at].astype(jnp.float32)
            value = value + (second + made[t])
            column = whole_row(source_of(m + heading * offsets[at]))
            value = value * inverses[jnp.minimum(column, 13)][0:1]
            out_ref[f, t] = jnp.where(f < count, value, 0.0)

    share.wait_send()
    for k in range(6):
        send_out(k).wait_send()
        pass_on(k).wait_send()


def shards(coupling, columns, row_slots):
    devices = lax.axis_size(AXIS)
    windows = [pltpu.VMEM((w, TILE, TILE), jnp.float32) for w in WIDTHS] * 3
    e_pool = pltpu.VMEM((ZERO + 1, TILE, TILE), jnp.bfloat16)
    f_pool = pltpu.VMEM((F_ZERO + 1, TILE, TILE), jnp.bfloat16)
    anywhere = pl.BlockSpec(memory_space=pl.ANY)
    by_tile = columns.T
    semaphore = pltpu.SemaphoreType.DMA
    return pl.pallas_call(
        functools.partial(kernel, devices),
        out_shape=pltpu.VMEM(coupling.shape, coupling.dtype),
        in_specs=[anywhere] * 3,
        out_specs=pl.BlockSpec(memory_space=pltpu.VMEM),
        scratch_shapes=[
            pltpu.VMEM(coupling.shape, jnp.float32),
            pltpu.VMEM(coupling.shape, jnp.float32),
            pltpu.SMEM(by_tile.shape, jnp.int32),
            pltpu.SMEM(row_slots.shape, jnp.int32),
        ]
        + windows
        + [e_pool, e_pool, f_pool, f_pool]
        + [
            pltpu.VMEM((14, 8, TILE), jnp.float32),
            pltpu.SMEM((SOURCES * SPAN,), jnp.int32),
            pltpu.SMEM((14 * TILES,), jnp.int32),
            pltpu.SMEM((F_ROWS,), jnp.int32),
            pltpu.SMEM((F_ROWS * NAMES,), jnp.int32),
            pltpu.SMEM((F_ROWS * NAMES,), jnp.int32),
        ]
        + [semaphore((6,))] * 4
        + [semaphore] * 5,
        compiler_params=pltpu.CompilerParams(collective_id=0, has_side_effects=True),
        name="iterate",
    )(coupling, by_tile, row_slots)


def solution(mesh):
    return jax.shard_map(
        shards,
        mesh=mesh,
        in_specs=(P(AXIS, None, None, None), P(), P()),
        out_specs=P(AXIS, None, None, None),
        check_vma=False,
    )
```

```python
import functools

import jax
import jax.numpy as jnp
from jax import lax
from jax.experimental import pallas as pl
from jax.experimental.pallas import tpu as pltpu
from jax.sharding import PartitionSpec as P

TILE = 128
TILES = 5
SLOT = 4
BAND = 3
AXIS = "rows"
RUN = 128
MESH = pl.DeviceIdType.MESH

WIDTHS = (5, 5, 5, 3, 2, 1)

WHOLE = 14 * TILES
PARTS = WIDTHS[3:]
ZERO = WHOLE + 2 * sum(PARTS)
SOURCES = 20
F_ROWS = 10
F_ZERO = F_ROWS * TILES
SPAN = 2 * BAND + 1
NAMES = TILES * TILES


def first_row(slots_ref, bound):
    found = jnp.int32(0)
    step = slots_ref.shape[0] // 2
    while step:
        below = slots_ref[found + step - 1] < bound
        found = found + jnp.where(below, step, 0)
        step //= 2
    return found


def held(slots_ref, start, device):
    rows = slots_ref.shape[0]
    count = jnp.int32(1)
    for k in range(1, SLOT):
        at = start + k
        inside = slots_ref[jnp.minimum(at, rows - 1)] < (device + 1) * SLOT
        count = count + jnp.where(jnp.logical_and(at < rows, inside), 1, 0)
    return count


def wrapped(value, rows):
    return lax.rem(value + rows, rows)


def signed(value, rows):
    half = rows // 2
    return lax.rem(value + rows + half, rows) - half


def inverse_column(tile, eye):
    return 1.0 / jnp.sum(jnp.where(eye, tile, 0.0), axis=1, keepdims=True)


def inverse_row(tile, eye):
    return 1.0 / jnp.sum(jnp.where(eye, tile, 0.0), axis=0, keepdims=True)


def split(value):
    high = value.astype(jnp.bfloat16)
    low = (value - high.astype(jnp.float32)).astype(jnp.bfloat16)
    return high, low


def dot(left, right):
    return jnp.dot(left, right, preferred_element_type=jnp.float32)


def multiply(left_high, left_low, base, pool_high, pool_low, names_ref, named):
    def block(pool, us, ts):
        return jnp.concatenate(
            [
                jnp.concatenate([pool[names_ref[named + u * TILES + t]] for t in ts], axis=1)
                for u in us
            ],
            axis=0,
        )

    def left(us):
        high = jnp.concatenate([left_high[base + u] for u in us], axis=1)
        low = jnp.concatenate([left_low[base + u] for u in us], axis=1)
        return high, jnp.concatenate([high, low], axis=0)

    pairs = ((0, 1), (2, 3))
    out = []
    for ts in pairs:
        total = None
        rest = None
        for us in pairs:
            high, both = left(us)
            part = dot(both, block(pool_high, us, ts))
            more = dot(high, block(pool_low, us, ts))
            total = part if total is None else total + part
            rest = more if rest is None else rest + more
        high = left_high[base + 4]
        low = left_low[base + 4]
        last = jnp.concatenate(
            [
                jnp.concatenate([high, high], axis=1),
                jnp.concatenate([low, jnp.zeros_like(low)], axis=1),
            ],
            axis=0,
        )
        right = jnp.concatenate([block(pool_high, (4,), ts), block(pool_low, (4,), ts)], axis=0)
        total = total + dot(last, right)
        value = total[:TILE] + total[TILE:] + rest
        out.append(value[:, :TILE])
        out.append(value[:, TILE:])
    total = None
    for us in pairs + ((4,),):
        right = jnp.concatenate([block(pool_high, us, (4,)), block(pool_low, us, (4,))], axis=1)
        part = dot(left(us)[1], right)
        total = part if total is None else total + part
    out.append(total[:TILE, :TILE] + (total[TILE:, :TILE] + total[:TILE, TILE:]))
    return out


def kernel(
    devices,
    own_hbm,
    columns_hbm,
    slots_hbm,
    out_ref,
    own_ref,
    partner_ref,
    columns_ref,
    slots_ref,
    *refs,
):
    leaving, arriving, passed = refs[0:6], refs[6:12], refs[12:18]
    e_high, e_low, f_high, f_low, inverses = refs[18:23]
    tiles, offsets, bases, names, f_names = refs[23:28]
    out_send, out_recv, pass_send, pass_recv, row_send, row_recv = refs[28:34]
    own_sem, columns_sem, slots_sem = refs[34:]
    rows = slots_ref.shape[0]
    me = lax.axis_index(AXIS)
    parity = lax.rem(me, 2)
    odd = parity == 1
    above, below = lax.rem(me + 2, devices), lax.rem(me + devices - 2, devices)
    outward = jnp.where(odd, above, below)
    partner = me + 1 - 2 * parity
    heading = 2 * parity - 1

    barrier = pltpu.get_barrier_semaphore()
    for other in (above, below, partner):
        pl.semaphore_signal(barrier, inc=1, device_id=(other,), device_id_type=MESH)
    fetch_slots = pltpu.make_async_copy(slots_hbm, slots_ref, slots_sem)
    fetch_slots.start()
    fetch = pltpu.make_async_copy(own_hbm, own_ref, own_sem)
    fetch.start()
    fetch_columns = pltpu.make_async_copy(columns_hbm, columns_ref, columns_sem)
    fetch_columns.start()

    shape = (TILE, TILE)
    eye = lax.broadcasted_iota(jnp.int32, shape, 0) == lax.broadcasted_iota(jnp.int32, shape, 1)

    fetch_slots.wait()
    chip_start = first_row(slots_ref, (me - parity) * SLOT)
    low_count = held(slots_ref, chip_start, me - parity)
    middle = chip_start + low_count
    high_count = held(slots_ref, middle, me - parity + 1)
    chip_end = middle + high_count
    start = jnp.where(odd, middle, chip_start)
    count = jnp.where(odd, high_count, low_count)
    partner_count = jnp.where(odd, low_count, high_count)
    partner_start = jnp.where(odd, chip_start, middle)


    def remote(source, target, send, recv, device):
        return pltpu.make_async_remote_copy(
            src_ref=source,
            dst_ref=target,
            send_sem=send,
            recv_sem=recv,
            device_id=(device,),
            device_id_type=MESH,
        )

    def send_out(k):
        return remote(leaving[k], arriving[k], out_send.at[k], out_recv.at[k], outward)

    def pass_on(k):
        return remote(arriving[k], passed[k], pass_send.at[k], pass_recv.at[k], partner)

    share = remote(own_ref, partner_ref, row_send, row_recv, partner)

    def row_of(source):
        if source < 4:
            row = start + source
        elif source < 8:
            row = partner_start + (source - 4)
        elif source < 14:
            k = source - 8
            row = jnp.where(odd, chip_start - 1 - k, chip_end + k)
        else:
            k = source - 14
            row = jnp.where(odd, chip_end + k, chip_start - 1 - k)
        return wrapped(row, rows)

    def whole_row(source):
        return jnp.where(source < 11, source, source - 3)

    def source_of(m):
        inner = -1 - m
        beyond = 8 + inner - partner_count
        beside = 4 + jnp.where(odd, partner_count - 1 - inner, inner)
        own = jnp.where(odd, m, count - 1 - m)
        outer = 14 + m - count
        near = jnp.where(inner < partner_count, beside, beyond)
        source = jnp.where(m < 0, near, jnp.where(m < count, own, outer))
        return jnp.clip(source, 0, SOURCES - 1)

    def f_row_of(m):
        own = jnp.where(odd, m, count - 1 - m)
        row = jnp.where(m < 0, 3 - m, jnp.where(m < count, own, 7 + m - count))
        return jnp.clip(row, 0, F_ROWS - 1)

    def own_slot(k):
        return jnp.where(odd, jnp.maximum(count - 1 - k, 0), k)

    def partner_slot(inner):
        return jnp.clip(jnp.where(odd, partner_count - 1 - inner, inner), 0, SLOT - 1)

    def fill_whole(k):
        inner = k - count
        for t in range(TILES):
            value = own_ref[own_slot(k), t]
            if k > 0:
                value = jnp.where(inner >= 0, partner_ref[partner_slot(inner), t], value)
            for j in range(k - 1):
                value = jnp.where(inner - partner_count == j, arriving[j][t], value)
            leaving[k][t] = value

    def tile_at_offset(row, offset):
        slot = slots_ref[row]
        target = wrapped(row + offset, rows)
        found = jnp.int32(0)
        for v in range(1, TILES):
            found = jnp.where(columns_ref[v, slot] == target, v, found)
        return found

    def fill_part(k):
        inner = k - count
        beyond = inner - partner_count
        row = wrapped(jnp.where(odd, chip_end - 1 - k, chip_start + k), rows)

        def pick(t):
            value = partner_ref[partner_slot(inner), t]
            if k < SLOT:
                value = jnp.where(inner < 0, own_ref[own_slot(k), t], value)
            for j in range(min(k - 1, 3)):
                value = jnp.where(beyond == j, arriving[j][t], value)
            return value

        scale = inverse_column(pick(0), eye)
        for place in range(WIDTHS[k]):
            offset = heading * (BAND - WIDTHS[k] + 1 + place)
            index = tile_at_offset(row, offset)
            value = jnp.where(index > 0, -(scale * pick(index)), 0.0)
            for j in range(3, k - 1):
                ready = arriving[j][WIDTHS[j] - WIDTHS[k] + place]
                value = jnp.where(beyond == j, ready, value)
            leaving[k][place] = value

    def forward(k):
        if k < 3:
            fill_whole(k)
        else:
            fill_part(k)
        send_out(k).start()

    def convert_whole(e):
        if e < 4:
            source = own_ref.at[e]
        elif e < 8:
            source = partner_ref.at[e - 4]
        else:
            source = arriving[e - 8] if e < 11 else passed[e - 11]
        diagonal = source[0]
        scale = inverse_column(diagonal, eye)
        inverses[e] = jnp.broadcast_to(inverse_row(diagonal, eye), (8, TILE))
        for v in range(TILES):
            value = -(scale * source[v])
            if v == 0:
                value = jnp.where(eye, 1.0, 0.0) + value
            e_high[e * TILES + v], e_low[e * TILES + v] = split(value)

    def part_index(side, k):
        return WHOLE + side * sum(PARTS) + sum(PARTS[: k - 3])

    def convert_part(side, k):
        at = part_index(side, k)
        for n in range(WIDTHS[k]):
            e_high[at + n], e_low[at + n] = split((arriving, passed)[side][k][n])

    fetch.wait()
    fill_whole(0)
    pl.semaphore_wait(barrier, 3)
    send_out(0).start()
    share.start()

    fetch_columns.wait()
    for e in range(14):
        source = e if e < 11 else e + 3
        row = row_of(source)
        slot = slots_ref[row]
        found = [jnp.int32(ZERO)] * SPAN
        found[BAND] = jnp.int32(e * TILES)
        offsets[e * TILES] = 0
        for v in range(1, TILES):
            offset = jnp.clip(signed(columns_ref[v, slot] - row, rows), -BAND, BAND)
            offsets[e * TILES + v] = offset
            for o in range(SPAN):
                if o != BAND:
                    found[o] = jnp.where(offset == o - BAND, e * TILES + v, found[o])
        for o in range(SPAN):
            tiles[source * SPAN + o] = found[o]
    for side in (0, 1):
        for k in range(3, 6):
            source = 8 + 6 * side + k
            for o in range(SPAN):
                tiles[source * SPAN + o] = ZERO
            for n in range(WIDTHS[k]):
                offset = heading * (1 - 2 * side) * (BAND - WIDTHS[k] + 1 + n)
                tiles[source * SPAN + BAND + offset] = part_index(side, k) + n

    zeros = jnp.zeros((TILE, TILE), jnp.bfloat16)
    e_high[ZERO] = zeros
    e_low[ZERO] = zeros
    f_high[F_ZERO] = zeros
    f_low[F_ZERO] = zeros
    for e in range(4):
        convert_whole(e)

    share.wait_recv()
    forward(1)

    def distance(f):
        own = jnp.where(odd, f, count - 1 - f)
        return jnp.where(f < 4, own, jnp.where(f < 7, 3 - f, count + f - 7))

    @pl.loop(0, F_ROWS)
    def _(f):
        m = distance(f)
        source = jnp.where(f < 4, f, source_of(m))
        base = whole_row(source) * TILES
        bases[f] = base
        for u in range(TILES):
            first = offsets[base + u]
            at = source_of(m + heading * first)
            shift = f_row_of(m + heading * first) * TILES - whole_row(at) * TILES
            for t in range(TILES):
                offset = offsets[base + t] - first
                near = jnp.logical_and(offset <= BAND, offset >= -BAND)
                name = tiles[at * SPAN + BAND + jnp.where(near, offset, 0)]
                name = jnp.where(near, name, ZERO)
                names[f * NAMES + u * TILES + t] = name
                moved = jnp.clip(name + shift, 0, F_ZERO - 1)
                f_names[f * NAMES + u * TILES + t] = jnp.where(name == ZERO, F_ZERO, moved)

    for e in range(4, 8):
        convert_whole(e)

    def square(f):
        made = multiply(e_high, e_low, bases[f], e_high, e_low, names, f * NAMES)
        for t in range(TILES):
            f_high[f * TILES + t], f_low[f * TILES + t] = split(made[t])

    def receive(k):
        send_out(k).wait_recv()
        pass_on(k).start()

    def take(k):
        pass_on(k).wait_recv()
        if k < 3:
            convert_whole(11 + k)
        else:
            convert_part(1, k)

    place = lax.rem(me, RUN)
    late = place < 4
    late_odd = jnp.logical_and(late, odd)
    late_even = jnp.logical_and(late, jnp.logical_not(odd))
    prompt = jnp.logical_not(late)
    not_late_even = jnp.logical_not(late_even)

    def squares(first, last):
        pl.loop(first, last)(square)

    def take_rows(condition, ks):
        @pl.when(condition)
        def _():
            for k in ks:
                take(k)

    def finish(f):
        made = multiply(e_high, e_low, f * TILES, f_high, f_low, f_names, f * NAMES)
        scale = inverse_column(own_ref[f, 0], eye)
        m = distance(f)
        for t in range(TILES):
            value = -(scale * own_ref[f, t])
            if t == 0:
                value = jnp.where(eye, 2.0, 0.0) + value
            at = f * TILES + t
            second = f_high[at].astype(jnp.float32) + f_low[at].astype(jnp.float32)
            value = value + (second + made[t])
            column = whole_row(source_of(m + heading * offsets[at]))
            value = value * inverses[jnp.minimum(column, 13)][0:1]
            out_ref[f, t] = jnp.where(f < count, value, 0.0)

    for k in range(2, 6):
        receive(k - 2)
        forward(k)
        if k < 5:
            convert_whole(6 + k)
        else:
            convert_part(0, 3)
        if k == 3:
            take_rows(late_odd, (0, 1, 2))
        if k > 2:
            take_rows(prompt, (k - 3,))
        if k == 4:
            squares(jnp.where(late_odd, 0, 4), jnp.where(late_even, 4, 5))

    @pl.when(late_even)
    def _():
        receive(4)
        convert_part(0, 4)
        receive(5)

    squares(6, jnp.where(late_even, 7, 6))
    take_rows(late_even, (0, 1))
    squares(jnp.where(late_even, 4, 5), 6)
    take_rows(late_even, (2,))
    squares(jnp.where(late_odd, 4, 0), 4)
    take(3)
    squares(7, 8)
    pl.loop(2, jnp.where(late_even, 4, 2))(finish)

    @pl.when(not_late_even)
    def _():
        receive(4)
        convert_part(0, 4)

    squares(jnp.where(late_even, 7, 6), 7)
    take(4)
    squares(8, 9)
    pl.loop(1, jnp.where(late_even, 2, 1))(finish)

    @pl.when(not_late_even)
    def _():
        receive(5)

    take(5)
    squares(9, 10)
    pl.loop(0, jnp.where(late_even, 1, 4))(finish)

    share.wait_send()
    for k in range(6):
        send_out(k).wait_send()
        pass_on(k).wait_send()


def shards(coupling, columns, row_slots):
    devices = lax.axis_size(AXIS)
    windows = [pltpu.VMEM((w, TILE, TILE), jnp.float32) for w in WIDTHS] * 3
    e_pool = pltpu.VMEM((ZERO + 1, TILE, TILE), jnp.bfloat16)
    f_pool = pltpu.VMEM((F_ZERO + 1, TILE, TILE), jnp.bfloat16)
    anywhere = pl.BlockSpec(memory_space=pl.ANY)
    by_tile = columns.T
    semaphore = pltpu.SemaphoreType.DMA
    return pl.pallas_call(
        functools.partial(kernel, devices),
        out_shape=pltpu.VMEM(coupling.shape, coupling.dtype),
        in_specs=[anywhere] * 3,
        out_specs=pl.BlockSpec(memory_space=pltpu.VMEM),
        scratch_shapes=[
            pltpu.VMEM(coupling.shape, jnp.float32),
            pltpu.VMEM(coupling.shape, jnp.float32),
            pltpu.SMEM(by_tile.shape, jnp.int32),
            pltpu.SMEM(row_slots.shape, jnp.int32),
        ]
        + windows
        + [e_pool, e_pool, f_pool, f_pool]
        + [
            pltpu.VMEM((14, 8, TILE), jnp.float32),
            pltpu.SMEM((SOURCES * SPAN,), jnp.int32),
            pltpu.SMEM((14 * TILES,), jnp.int32),
            pltpu.SMEM((F_ROWS,), jnp.int32),
            pltpu.SMEM((F_ROWS * NAMES,), jnp.int32),
            pltpu.SMEM((F_ROWS * NAMES,), jnp.int32),
        ]
        + [semaphore((6,))] * 4
        + [semaphore] * 5,
        compiler_params=pltpu.CompilerParams(collective_id=0, has_side_effects=True),
        name="iterate",
    )(coupling, by_tile, row_slots)


def solution(mesh):
    return jax.shard_map(
        shards,
        mesh=mesh,
        in_specs=(P(AXIS, None, None, None), P(), P()),
        out_specs=P(AXIS, None, None, None),
        check_vma=False,
    )
```
